32 devices in a mesh: dp: 2 (over x), cp: 16 (over z, y, core).
Axes of the slice: x: 2, y: 2, z: 4, core: 2. Of those that a mesh axis runs over, the one named last changes fastest.
Arguments:
- x: bfloat16 [8192, 4096], P(('dp', 'cp')), parts along dimension 0
- seg: int32 [8192], P(('dp', 'cp')), parts along dimension 0
- wq: bfloat16 [4096, 4096], replicated
- wk: bfloat16 [4096, 1024], replicated
- wv: bfloat16 [4096, 1024], replicated
- wo: bfloat16 [4096, 4096], replicated
Outputs:
- output: bfloat16 [8192, 4096], P(('dp', 'cp')), parts along dimension 0
There are 2 independent parts. The reference program is written for one: setup_inputs(seed, part) draws one part's arguments, and reference() takes and returns one part's arrays. A program takes and returns all parts, laid end to end along the dimension named above; an argument that names none is the same for every part.
All inputs are finite; a program needn't handle non-finite values.
Results may differ from the reference program's by a relative error of at most 0.00590055.
Values are sent between devices in bfloat16 or wider.
A program may use at most 1 GiB of HBM per device.

```python
import jax
import jax.numpy as jnp
from jax import lax
import numpy as np

CP = 16
L = 256
D = 4096
HQ = 32
HKV = 8
DH = 128

S = CP * L
HALF = L // 2
G = HQ // HKV
QB = min(128, HALF)


def row_positions():
    rows = []
    for d in range(CP):
        rows.append(np.arange(d * HALF, (d + 1) * HALF))
        rows.append(np.arange((2 * CP - 1 - d) * HALF, (2 * CP - d) * HALF))
    return np.concatenate(rows).astype(np.int32)


def setup_inputs(seed: int = 0, part: int = 0) -> dict:
    key = jax.random.key(seed)
    kshared, kpart = jax.random.split(key)
    kp = jax.random.fold_in(kpart, part)
    kx, _, _ = jax.random.split(kp, 3)
    kd = jax.random.fold_in(kp, 7)
    ku, kc, kl = jax.random.split(kd, 3)
    kq, kk, kv, ko = jax.random.split(kshared, 4)
    x = jax.random.normal(kx, (S, D), jnp.float32).astype(jnp.bfloat16)
    token_pos = jnp.arange(S, dtype=jnp.int32)
    long_end = jax.random.randint(kl, (), 3 * S // 10, 7 * S // 10, jnp.int32)
    coin_flip = jax.random.randint(kc, (2 * CP,), 0, 2, jnp.int32)
    break_bar = jnp.repeat(jnp.where(coin_flip == 0, jnp.int32(1 << 22), jnp.int32((1 << 24) // L)), HALF)
    draw_bits = (jax.random.bits(ku, (S,), jnp.uint32) >> 8).astype(jnp.int32)
    breaks = (draw_bits < break_bar) & (token_pos > long_end)
    seg_orig = 7 + jnp.cumsum(breaks.astype(jnp.int32))
    seg = seg_orig[jnp.asarray(row_positions())].astype(jnp.int32)
    wq = (jax.random.normal(kq, (D, HQ * DH), jnp.float32) * (2.0 * D ** -0.5)).astype(jnp.bfloat16)
    wk = (jax.random.normal(kk, (D, HKV * DH), jnp.float32) * D ** -0.5).astype(jnp.bfloat16)
    wv = (jax.random.normal(kv, (D, HKV * DH), jnp.float32) * D ** -0.5).astype(jnp.bfloat16)
    wo = (jax.random.normal(ko, (HQ * DH, D), jnp.float32) * (HQ * DH) ** -0.5).astype(jnp.bfloat16)
    return {"x": x, "seg": seg, "wq": wq, "wk": wk, "wv": wv, "wo": wo}


def reference(x, seg, wq, wk, wv, wo):
    pos = jnp.asarray(row_positions())
    q = jnp.dot(x, wq, preferred_element_type=jnp.float32).astype(jnp.bfloat16)
    k = jnp.dot(x, wk, preferred_element_type=jnp.float32).astype(jnp.bfloat16)
    v = jnp.dot(x, wv, preferred_element_type=jnp.float32).astype(jnp.bfloat16)
    kf = k.astype(jnp.float32).reshape(S, HKV, DH)
    vf = v.astype(jnp.float32).reshape(S, HKV, DH)
    qb = q.reshape(S // QB, QB, HKV, G, DH)
    pb = pos.reshape(S // QB, QB)
    sb = seg.reshape(S // QB, QB)

    def block(args):
        qi, pi, si = args
        s = jnp.einsum("qhgd,khd->hgqk", qi.astype(jnp.float32), kf) * DH ** -0.5
        allowed = (si[:, None] == seg[None, :]) & (pos[None, :] <= pi[:, None])
        s = jnp.where(allowed, s, -jnp.inf)
        p = jax.nn.softmax(s, axis=-1)
        o = jnp.einsum("hgqk,khd->qhgd", p, vf)
        return o.astype(jnp.bfloat16)

    o = lax.map(block, (qb, pb, sb)).reshape(S, HQ * DH)
    return jnp.dot(o, wo, preferred_element_type=jnp.float32).astype(jnp.bfloat16)
```

```python
import functools
import math

import jax
import jax.numpy as jnp
from jax import lax
from jax.experimental import pallas as pl
from jax.experimental.pallas import tpu as pltpu
from jax.sharding import PartitionSpec as P

DH = 128
NKV = 8
G = 4
PIECE = 128
CH = 4 * PIECE
SCALE = math.log2(math.e) / math.sqrt(DH)
NEG = -1e30


def _bias(segq_row, segk_rows, qp, kps):
    sq = jnp.transpose(jnp.broadcast_to(segq_row, (PIECE, PIECE)))
    rows = lax.broadcasted_iota(jnp.int32, (PIECE, PIECE), 0) + qp * PIECE
    lanes = lax.broadcasted_iota(jnp.int32, (PIECE, PIECE), 1)
    out = []
    for sk, kp in zip(segk_rows, kps):
        ok = (sq == sk) & (lanes + kp * PIECE <= rows)
        out.append(jnp.where(ok, 0.0, NEG))
    return jnp.concatenate(out, axis=1)


def _attn_kernel(q_ref, kv_ref, segq_ref, segk_ref, o_ref, bias_ref, m_ref, l_ref, acc_ref, *, me_fn):
    me = me_fn()
    z = me // 4
    h = pl.program_id(0)

    def chunk_of(step):
        lo = step <= z
        t = step - (z + 1)
        c_lo = jnp.where(step == 0, z, step - 1)
        c_hi = jnp.where(t == 0, 4 + z, jnp.where(t <= 4, t - 1, z + t))
        return lo, jnp.where(lo, c_lo, c_hi)

    @pl.when(h == 0)
    def _():
        def body(step, _):
            lo, c = chunk_of(step)
            qi = jnp.where(lo, 0, 1)
            qp = jnp.where(lo, me, 31 - me)
            hi = jnp.where(c >= 4, 1, 0)
            segk, kps = [], []
            for j in range(4):
                dev = 4 * (c - 4 * hi) + j
                segk.append(segk_ref[dev, pl.ds(hi, 1), :])
                kps.append(jnp.where(hi == 1, 31 - dev, dev))
            bias_ref[step] = _bias(segq_ref[pl.ds(qi, 1), :], segk, qp, kps)
            return 0
        lax.fori_loop(0, 9, body, 0)

    def piece(first, count, row0):
        m_ref[...] = jnp.full_like(m_ref, -jnp.inf)
        l_ref[...] = jnp.zeros_like(l_ref)
        acc_ref[...] = jnp.zeros_like(acc_ref)

        def body(i, _):
            step = first + i
            _, c = chunk_of(step)
            hi = jnp.where(c >= 4, 1, 0)
            dev = 4 * (c - 4 * hi)
            k = kv_ref[pl.ds(dev, 4), hi, 0, 0].reshape(CH, DH)
            v = kv_ref[pl.ds(dev, 4), hi, 0, 1].reshape(CH, DH)
            for g in range(G):
                q = q_ref[row0:row0 + PIECE, g * DH:(g + 1) * DH]
                s = lax.dot_general(q, k, (((1,), (1,)), ((), ())), preferred_element_type=jnp.float32)
                s = s * SCALE + bias_ref[step]
                m_old = m_ref[g]
                m_new = jnp.maximum(m_old, jnp.max(s, axis=1, keepdims=True))
                p = jnp.exp2(s - m_new[:, :1])
                corr = jnp.exp2(m_old - m_new)
                l_ref[g] = l_ref[g] * corr + jnp.sum(p, axis=1, keepdims=True)
                pv = lax.dot_general(p.astype(jnp.bfloat16), v, (((1,), (0,)), ((), ())), preferred_element_type=jnp.float32)
                acc_ref[g] = acc_ref[g] * corr + pv
                m_ref[g] = m_new
            return 0
        lax.fori_loop(0, count, body, 0)
        for g in range(G):
            o_ref[row0:row0 + PIECE, g * DH:(g + 1) * DH] = (acc_ref[g] / l_ref[g]).astype(jnp.bfloat16)

    piece(0, z + 1, 0)
    piece(z + 1, 8 - z, PIECE)


def solution(mesh):
    n = mesh.shape["cp"]

    def local(x, seg, wq, wk, wv, wo):
        k = jnp.dot(x, wk, preferred_element_type=jnp.float32).astype(jnp.bfloat16)
        v = jnp.dot(x, wv, preferred_element_type=jnp.float32).astype(jnp.bfloat16)
        kv = jnp.stack([k.reshape(2, PIECE, NKV, DH), v.reshape(2, PIECE, NKV, DH)], axis=0)
        kv = jnp.transpose(kv, (1, 3, 0, 2, 4))
        kv_all = lax.all_gather(kv, "cp", axis=0, tiled=False)
        segk = lax.all_gather(seg.reshape(2, PIECE), "cp", axis=0, tiled=False)
        q = jnp.dot(x, wq, preferred_element_type=jnp.float32).astype(jnp.bfloat16)
        o = pl.pallas_call(
            functools.partial(_attn_kernel, me_fn=lambda: lax.axis_index("cp")),
            out_shape=jax.ShapeDtypeStruct((2 * PIECE, NKV * G * DH), jnp.bfloat16),
            grid=(NKV,),
            in_specs=[
                pl.BlockSpec((2 * PIECE, G * DH), lambda h: (0, h)),
                pl.BlockSpec((n, 2, 1, 2, PIECE, DH), lambda h: (0, 0, h, 0, 0, 0)),
                pl.BlockSpec((2, PIECE), lambda h: (0, 0)),
                pl.BlockSpec((n, 2, PIECE), lambda h: (0, 0, 0)),
            ],
            out_specs=pl.BlockSpec((2 * PIECE, G * DH), lambda h: (0, h)),
            scratch_shapes=[
                pltpu.VMEM((9, PIECE, CH), jnp.float32),
                pltpu.VMEM((G, PIECE, DH), jnp.float32),
                pltpu.VMEM((G, PIECE, DH), jnp.float32),
                pltpu.VMEM((G, PIECE, DH), jnp.float32),
            ],
            cost_estimate=pl.CostEstimate(flops=10_000_000_000, bytes_accessed=20_000_000, transcendentals=0),
        )(q, kv_all, seg.reshape(2, PIECE), segk)
        return jnp.dot(o, wo, preferred_element_type=jnp.float32).astype(jnp.bfloat16)

    rows = P(("dp", "cp"), None)
    return jax.shard_map(local, mesh=mesh, in_specs=(rows, P(("dp", "cp")), P(), P(), P(), P()), out_specs=rows, check_vma=False)
```

```python
import functools
import math

import jax
import jax.numpy as jnp
from jax import lax
from jax.experimental import pallas as pl
from jax.experimental.pallas import tpu as pltpu
from jax.sharding import PartitionSpec as P

DH = 128
NKV = 8
G = 4
PIECE = 128
CH = 4 * PIECE
R = G * PIECE
D = 4096
SCALE = math.log2(math.e) / math.sqrt(DH)
NEG = -1e30
MESH = pl.DeviceIdType.MESH
NWB = 5
N_SEND = (12, 15, 20, 17)
N_RECV = ((3, 4, 6, 4), (1, 2, 4, 3), (0, 0, 0, 1), (6, 8, 12, 10))


def _dot_t(a, b):
    return lax.dot_general(a, b, (((1,), (1,)), ((), ())), preferred_element_type=jnp.float32)


def _dot(a, b):
    return lax.dot_general(a, b, (((1,), (0,)), ((), ())), preferred_element_type=jnp.float32)


def _chunk_of(z, n):
    t = n - (z + 1)
    c_lo = jnp.where(n == 0, z, n - 1)
    c_far = jnp.where(t == 0, 4, jnp.where(t <= 4, t - 1, 5))
    c_near = jnp.where(t == 1, 5, 4)
    lo = t < 0
    c = jnp.where(lo, c_lo, jnp.where(z >= 2, c_far, c_near))
    return jnp.where(lo, 0, 1), c, (z >= 2) | (t <= 1)


def _mask(out_ref, me, own, low_query, seg_ref, dev, low_key, valid=True):
    def pick(low, both):
        return jnp.where(low, both[:1], both[1:])
    def piece(low, d):
        return jnp.where(low, d, 31 - d) * PIECE
    shape = (PIECE, PIECE)
    sq = jnp.transpose(jnp.broadcast_to(pick(low_query, own), shape))
    rows = lax.broadcasted_iota(jnp.int32, shape, 0) + piece(low_query, me)
    lanes = lax.broadcasted_iota(jnp.int32, shape, 1)
    for j in range(4):
        ok = (sq == pick(low_key, seg_ref[dev + j])) & (lanes + piece(low_key, dev + j) <= rows) & valid
        out_ref[:, j * PIECE:(j + 1) * PIECE] = jnp.where(ok, 0.0, NEG)


def _fused_kernel(x_ref, seg_ref, wk_ref, wv_ref, wq_ref, wo_ref, y_ref, flag_ref,
                  kv_ref, q_ref, w_ref, s_ref, bias_ref, m_ref, l_ref, acc_ref, yacc_ref, o_ref,
                  seg_all, seg_other, ssem, rsem, wsem, seg_lsem, seg_ssem, seg_rsem, seg_osem):
    me = lax.axis_index("cp")
    dp = lax.axis_index("dp")
    z = me // 4
    y = (me // 2) % 2
    c = me % 2
    yb = 1 - y
    to_y = 4 * z + 2 * yb + c
    to_c = 4 * z + 2 * y + (1 - c)

    def tile_copies(t):
        slot = lax.rem(t, NWB)
        buf, sem = w_ref.at[slot], wsem.at[slot]
        def kv_tile():
            return [pltpu.make_async_copy(w.at[:, pl.ds(pl.multiple_of(256 * t, 256), 256)], buf.at[:, pl.ds(256 * i, 256)], sem)
                    for i, w in enumerate((wk_ref, wv_ref))]
        def q_tile():
            return [pltpu.make_async_copy(wq_ref.at[:, pl.ds(pl.multiple_of(512 * (t - 4), 512), 512)], buf, sem)]
        def o_tile():
            return [pltpu.make_async_copy(wo_ref.at[pl.ds(pl.multiple_of(512 * (t - 12), 512), 512), pl.ds(512 * j, 512)],
                                          buf.at[pl.ds(512 * j, 512), :], sem) for j in range(8)]
        return kv_tile, q_tile, o_tile

    def start_tile(t):
        kv_tile, q_tile, o_tile = tile_copies(t)
        @pl.when(t < 4)
        def _():
            for cp in kv_tile():
                cp.start()
        @pl.when((t >= 4) & (t < 12))
        def _():
            for cp in q_tile():
                cp.start()
        @pl.when((t >= 12) & (t < 20))
        def _():
            for cp in o_tile():
                cp.start()

    def wait_tile(t):
        slot = lax.rem(t, NWB)
        pltpu.make_async_copy(wq_ref.at[:, pl.ds(0, 512)], w_ref.at[slot], wsem.at[slot]).wait()

    own_seg = pltpu.make_async_copy(seg_ref, seg_all.at[me], seg_lsem)
    own_seg.start()
    for t in range(NWB):
        start_tile(jnp.int32(t))

    barrier = pltpu.get_barrier_semaphore()
    for i in range(1, 16):
        pl.semaphore_signal(barrier, inc=1, device_id={"cp": lax.rem(me + i, 16)}, device_id_type=MESH)
    pl.semaphore_signal(barrier, inc=1, device_id={"dp": 1 - dp}, device_id_type=MESH)

    def enter(_):
        pl.semaphore_wait(barrier, 16)

    def share_seg(_):
        own_seg.wait()
        for i in range(1, 16):
            pltpu.make_async_remote_copy(src_ref=seg_all.at[me], dst_ref=seg_all.at[me], send_sem=seg_ssem, recv_sem=seg_rsem,
                                         device_id={"cp": lax.rem(me + i, 16)}, device_id_type=MESH).start()

    seg_swap = pltpu.make_async_remote_copy(src_ref=seg_all, dst_ref=seg_other, send_sem=seg_osem.at[0], recv_sem=seg_osem.at[1],
                                            device_id={"dp": 1 - dp}, device_id_type=MESH)

    def low(k, yy):
        return 4 * k + 2 * yy + c
    def own_high(yy):
        return 16 + 2 * yy + c
    def up_high(yy):
        return 20 + 2 * yy + c

    def send(h, stage, target, src, dst=None):
        dst = src if dst is None else dst
        pltpu.make_async_remote_copy(src_ref=kv_ref.at[h, src], dst_ref=kv_ref.at[h, dst], send_sem=ssem.at[h],
                                     recv_sem=rsem.at[h, stage], device_id={"cp": target}, device_id_type=MESH).start()

    def mate(h, *items):
        for i in items:
            send(h, 3, to_c, i)

    def t0(h):
        @pl.when(z == 0)
        def _():
            send(h, 0, me + 12, low(0, y))
            send(h, 0, me + 8, low(0, y))
            send(h, 0, me + 4, low(0, y))
            send(h, 0, to_y, low(0, y))
            send(h, 0, to_y, own_high(y))
            mate(h, low(0, y), own_high(y))
        for zz in (1, 2):
            @pl.when(z == zz)
            def _():
                send(h, 0, me + 4, low(zz, y))
                send(h, 0, to_y, low(zz, y))
                send(h, 0, to_y, own_high(y))
                send(h, 0, me - 4, own_high(y), up_high(y))
                mate(h, low(zz, y), own_high(y))
        @pl.when(z == 3)
        def _():
            send(h, 0, me - 4, low(3, y))
            send(h, 0, to_y, low(3, y))
            send(h, 0, to_y, own_high(y))
            send(h, 0, me - 4, own_high(y), up_high(y))
            mate(h, low(3, y), own_high(y))

    def arrive(h, stage):
        for zz in range(4):
            n = N_RECV[stage][zz]
            if n:
                @pl.when(z == zz)
                def _():
                    pltpu.make_async_copy(kv_ref.at[h, pl.ds(0, n)], kv_ref.at[h, pl.ds(0, n)], rsem.at[h, stage]).wait()

    def w1(h):
        arrive(h, 0)
        @pl.when(z == 0)
        def _():
            send(h, 1, to_y, up_high(y))
            mate(h, low(0, yb), own_high(yb), up_high(y))
        @pl.when(z == 1)
        def _():
            send(h, 1, me + 4, low(1, yb))
            send(h, 1, to_y, low(0, y))
            send(h, 1, to_y, up_high(y))
            mate(h, low(1, yb), own_high(yb), low(0, y), up_high(y))
        @pl.when(z == 2)
        def _():
            send(h, 1, me + 4, low(1, y))
            send(h, 1, me + 4, low(2, yb))
            send(h, 1, to_y, low(0, y))
            send(h, 1, to_y, up_high(y))
            mate(h, low(2, yb), low(1, y), low(0, y), up_high(y), own_high(yb), low(3, y))
        @pl.when(z == 3)
        def _():
            send(h, 1, to_y, low(0, y))
            send(h, 1, me - 4, low(3, yb))
            mate(h, low(0, y), low(3, yb), own_high(yb), low(2, y))

    def w2(h):
        arrive(h, 1)
        @pl.when(z == 0)
        def _():
            mate(h, up_high(yb))
        @pl.when(z == 1)
        def _():
            mate(h, low(0, yb), up_high(yb))
        @pl.when(z == 2)
        def _():
            mate(h, low(1, yb), low(3, yb), low(0, yb), up_high(yb))
        @pl.when(z == 3)
        def _():
            send(h, 2, to_y, low(1, y))
            mate(h, low(1, y), low(2, yb), low(0, yb))

    def w3(h):
        arrive(h, 2)
        @pl.when(z == 3)
        def _():
            mate(h, low(1, yb))

    def w4(h):
        arrive(h, 3)

    def kv_step(t):
        wait_tile(t)
        r = _dot(x_ref[...], w_ref[lax.rem(t, NWB)]).astype(jnp.bfloat16)
        for sel, slot in ((0, low(z, y)), (1, own_high(y))):
            for i in range(2):
                for j in range(2):
                    kv_ref[2 * t + i, slot, j] = r[sel * PIECE:(sel + 1) * PIECE, 256 * j + 128 * i:256 * j + 128 * (i + 1)]
        start_tile(t + NWB)

    def kv_body(t, _):
        kv_step(t)
        run(kv_plan, t)
        return 0

    def run(plan, i):
        for when, *what in plan:
            @pl.when(i == when)
            def _():
                for fn, head in what:
                    fn(head)

    kv_plan = (
        (0, (enter, 0), (t0, 0), (t0, 1), (share_seg, 0)),
        (1, (t0, 2)),
        (3, (w1, 0)),
    )
    lax.fori_loop(0, 4, kv_body, 0)

    def make_bias(_):
        pltpu.make_async_copy(seg_all.at[pl.ds(0, 15)], seg_all.at[pl.ds(0, 15)], seg_rsem).wait()
        seg_swap.start()
        own = seg_all[me]
        def body(n, _):
            sel, ck, valid = _chunk_of(z, n)
            low_key = ck < 4
            dev = jnp.where(low_key, 4 * ck, jnp.minimum(4 * (z + ck - 4), 12))
            _mask(bias_ref.at[n], me, own, sel == 0, seg_all, dev, low_key, valid)
            return 0
        lax.fori_loop(0, 3 * groups, body, 0)

    groups = jnp.where(z >= 2, 3, z + 1)

    def q_body(j, _):
        t = j + 4
        wait_tile(t)
        r = _dot(x_ref[...], w_ref[lax.rem(t, NWB)]).astype(jnp.bfloat16)
        for sel in range(2):
            for g in range(G):
                q_ref[j, sel, g * PIECE:(g + 1) * PIECE, :] = r[sel * PIECE:(sel + 1) * PIECE, g * DH:(g + 1) * DH]
        start_tile(t + NWB)
        run(q_plan, j)
        return 0

    q_plan = (
        (0, (t0, 3)),
        (2, (w1, 1)),
        (3, (w2, 0), (make_bias, 0)),
        (4, (t0, 4)),
        (5, (w3, 0), (w1, 2)),
        (6, (w2, 1)),
    )

    lax.fori_loop(0, 8, q_body, 0)

    def score(h, n):
        sel, ck, _ = _chunk_of(z, n)
        k = kv_ref[h, pl.ds(4 * ck, 4), 0].reshape(CH, DH)
        s = _dot_t(q_ref[h, sel], k)
        s = (s.reshape(G, PIECE, CH) * SCALE + bias_ref[n][None]).reshape(R, CH)
        s_ref[n] = s
        s = [s[:, i * DH:(i + 1) * DH] for i in range(4)]
        m_ref[sel] = jnp.maximum(m_ref[sel], functools.reduce(jnp.maximum, s))

    def weigh(h, n):
        sel, ck, _ = _chunk_of(z, n)
        v = kv_ref[h, pl.ds(4 * ck, 4), 1].reshape(CH, DH)
        m = m_ref[sel]
        p = [jnp.exp2(s_ref[n, :, i * DH:(i + 1) * DH] - m) for i in range(4)]
        l_ref[sel] = l_ref[sel] + functools.reduce(jnp.add, p)
        pb = jnp.concatenate([a.astype(jnp.bfloat16) for a in p], axis=1)
        acc_ref[sel] = acc_ref[sel] + _dot(pb, v)

    def steps(fn, h):
        def group(i, _):
            for u in range(3):
                fn(h, 3 * i + u)
            return 0
        lax.fori_loop(0, groups, group, 0)

    def project(t, last):
        slots = lax.rem(t, NWB), lax.rem(t + 1, NWB)
        for j in range(8):
            cols = slice(R * j, R * (j + 1))
            r = _dot(o_ref[0], w_ref[slots[0], cols, :]) + _dot(o_ref[1], w_ref[slots[1], cols, :])
            if last:
                y_ref[:, cols] = (yacc_ref[:, cols] + r).astype(jnp.bfloat16)
            else:
                yacc_ref[:, cols] = yacc_ref[:, cols] + r
        start_tile(t + NWB)
        start_tile(t + 1 + NWB)

    def attend(h, half, last=False):
        def ahead(n, fn):
            @pl.when(h + n < NKV)
            def _():
                fn(h + n)
        if not last:
            ahead(5, t0)
            ahead(3, w1)
            ahead(1, w3)
        w4(h)
        m_ref[...] = jnp.full_like(m_ref, -jnp.inf)
        l_ref[...] = jnp.zeros_like(l_ref)
        acc_ref[...] = jnp.zeros_like(acc_ref)
        steps(score, h)
        if not last:
            ahead(2, w2)
        for sel in range(2):
            m_ref[sel] = jnp.broadcast_to(jnp.max(m_ref[sel], axis=1, keepdims=True), (R, DH))
        steps(weigh, h)
        t = h + 11
        if half:
            wait_tile(t)
            wait_tile(t + 1)
        for sel in range(2):
            a = (acc_ref[sel] / jnp.sum(l_ref[sel], axis=1, keepdims=True)).astype(jnp.bfloat16)
            for g in range(G):
                o_ref[half, sel * PIECE:(sel + 1) * PIECE, g * DH:(g + 1) * DH] = a[g * PIECE:(g + 1) * PIECE]
        if half:
            project(t, last)

    yacc_ref[...] = jnp.zeros_like(yacc_ref)

    def pair(i, _):
        attend(2 * i, 0)
        attend(2 * i + 1, 1)
        return 0
    lax.fori_loop(0, 3, pair, 0)
    attend(jnp.int32(6), 0)
    attend(jnp.int32(7), 1, last=True)

    seg_swap.wait()
    def reach(ref):
        def first(d):
            return jnp.broadcast_to(ref[d][1:2, 0:1], (1, PIECE))
        def last_(d):
            return jnp.broadcast_to(ref[d][1:2, PIECE - 1:PIECE], (1, PIECE))
        return (first(7) == last_(12)) | (first(3) == last_(8))
    flag_ref[...] = jnp.where(reach(seg_all) | reach(seg_other), 1, 0)

    pltpu.make_async_copy(seg_all.at[pl.ds(0, 15)], seg_all.at[pl.ds(0, 15)], seg_ssem).wait()
    def drain(h, _):
        for zz in range(4):
            @pl.when(z == zz)
            def _():
                ref = kv_ref.at[h, pl.ds(0, N_SEND[zz])]
                pltpu.make_async_copy(ref, ref, ssem.at[h]).wait()
        return 0
    lax.fori_loop(0, NKV, drain, 0)


def _fused(x, seg, wq, wk, wv, wo):
    vmem = pl.BlockSpec(memory_space=pltpu.VMEM)
    hbm = pl.BlockSpec(memory_space=pl.ANY)
    dma = pltpu.SemaphoreType.DMA
    return pl.pallas_call(
        _fused_kernel,
        out_shape=(jax.ShapeDtypeStruct((2 * PIECE, D), jnp.bfloat16), jax.ShapeDtypeStruct((1, PIECE), jnp.int32)),
        in_specs=[vmem, hbm, hbm, hbm, hbm, hbm],
        out_specs=(vmem, vmem),
        scratch_shapes=[
            pltpu.VMEM((NKV, 24, 2, PIECE, DH), jnp.bfloat16),
            pltpu.VMEM((NKV, 2, R, DH), jnp.bfloat16),
            pltpu.VMEM((NWB, D, 512), jnp.bfloat16),
            pltpu.VMEM((9, R, CH), jnp.float32),
            pltpu.VMEM((9, PIECE, CH), jnp.float32),
            pltpu.VMEM((2, R, DH), jnp.float32),
            pltpu.VMEM((2, R, DH), jnp.float32),
            pltpu.VMEM((2, R, DH), jnp.float32),
            pltpu.VMEM((2 * PIECE, D), jnp.float32),
            pltpu.VMEM((2, 2 * PIECE, R), jnp.bfloat16),
            pltpu.VMEM((16, 2, PIECE), jnp.int32),
            pltpu.VMEM((16, 2, PIECE), jnp.int32),
            dma((NKV,)),
            dma((NKV, 4)),
            dma((NWB,)),
            dma, dma, dma,
            dma((2,)),
        ],
        compiler_params=pltpu.CompilerParams(collective_id=0, has_side_effects=True, vmem_limit_bytes=67043328),
        cost_estimate=pl.CostEstimate(flops=30_000_000_000, bytes_accessed=90_000_000, transcendentals=0),
    )(x, seg.reshape(2, PIECE), wk, wv, wq, wo)


def _chunk_any(z, n):
    lo = n <= z
    t = n - (z + 1)
    c_lo = jnp.where(n == 0, z, n - 1)
    c_hi = jnp.where(t == 0, 4 + z, jnp.where(t <= 4, t - 1, z + t))
    return lo, jnp.where(lo, c_lo, c_hi)


def _any_kernel(q_ref, kv_ref, seg_ref, o_ref, bias_ref, m_ref, l_ref, acc_ref):
    me = lax.axis_index("cp")
    z = me // 4
    m_ref[...] = jnp.full_like(m_ref, -jnp.inf)
    l_ref[...] = jnp.zeros_like(l_ref)
    acc_ref[...] = jnp.zeros_like(acc_ref)
    own = seg_ref[me]

    def body(n, _):
        lo, ck = _chunk_any(z, n)
        sel = jnp.where(lo, 0, 1)
        hi = jnp.where(ck >= 4, 1, 0)
        dev0 = 4 * (ck - 4 * hi)
        _mask(bias_ref, me, own, lo, seg_ref, dev0, hi == 0)
        k = kv_ref[pl.ds(dev0, 4), hi, 0, 0].reshape(CH, DH)
        v = kv_ref[pl.ds(dev0, 4), hi, 0, 1].reshape(CH, DH)
        for g in range(G):
            i = sel * G + g
            s = _dot_t(q_ref[sel, 0, g], k) * SCALE + bias_ref[...]
            m_old = m_ref[i]
            m_new = jnp.maximum(m_old, jnp.max(s, axis=1, keepdims=True))
            p = jnp.exp2(s - m_new[:, :1])
            corr = jnp.exp2(m_old - m_new)
            l_ref[i] = l_ref[i] * corr + jnp.sum(p, axis=1, keepdims=True)
            acc_ref[i] = acc_ref[i] * corr + _dot(p.astype(jnp.bfloat16), v)
            m_ref[i] = m_new
        return 0
    lax.fori_loop(0, 9, body, 0)
    for sel in range(2):
        for g in range(G):
            o_ref[sel, 0, g] = (acc_ref[sel * G + g] / l_ref[sel * G + g]).astype(jnp.bfloat16)


def _general(x, seg, wq, wk, wv, wo, n):
    perm = [(j, (j + 1) % n) for j in range(n)]
    k = jnp.dot(x, wk, preferred_element_type=jnp.float32).astype(jnp.bfloat16)
    v = jnp.dot(x, wv, preferred_element_type=jnp.float32).astype(jnp.bfloat16)
    kv = jnp.stack([k.reshape(2, PIECE, NKV, DH), v.reshape(2, PIECE, NKV, DH)], axis=0)
    kv = jnp.transpose(kv, (1, 3, 0, 2, 4))
    seg = seg.reshape(2, PIECE)
    me = lax.axis_index("cp")

    def body(i, carry):
        kv, sg, kv_all, sg_all = carry
        src = (me - i) % n
        kv_all = lax.dynamic_update_index_in_dim(kv_all, kv, src, 0)
        sg_all = lax.dynamic_update_index_in_dim(sg_all, sg, src, 0)
        return lax.ppermute(kv, "cp", perm), lax.ppermute(sg, "cp", perm), kv_all, sg_all
    init = (kv, seg, jnp.zeros((n,) + kv.shape, kv.dtype), jnp.zeros((n,) + seg.shape, seg.dtype))
    _, _, kv_all, seg_all = lax.fori_loop(0, n, body, init)
    q = jnp.dot(x, wq, preferred_element_type=jnp.float32).astype(jnp.bfloat16)
    q = jnp.transpose(q.reshape(2, PIECE, NKV, G, DH), (0, 2, 3, 1, 4))
    o = pl.pallas_call(
        _any_kernel,
        out_shape=jax.ShapeDtypeStruct((2, NKV, G, PIECE, DH), jnp.bfloat16),
        grid=(NKV,),
        in_specs=[
            pl.BlockSpec((2, 1, G, PIECE, DH), lambda h: (0, h, 0, 0, 0)),
            pl.BlockSpec((n, 2, 1, 2, PIECE, DH), lambda h: (0, 0, h, 0, 0, 0)),
            pl.BlockSpec((n, 2, PIECE), lambda h: (0, 0, 0)),
        ],
        out_specs=pl.BlockSpec((2, 1, G, PIECE, DH), lambda h: (0, h, 0, 0, 0)),
        scratch_shapes=[pltpu.VMEM((PIECE, CH), jnp.float32)] + [pltpu.VMEM((2 * G, PIECE, DH), jnp.float32)] * 3,
    )(q, kv_all, seg_all)
    o = jnp.transpose(o, (0, 3, 1, 2, 4)).reshape(2 * PIECE, NKV * G * DH)
    return jnp.dot(o, wo, preferred_element_type=jnp.float32).astype(jnp.bfloat16)


def solution(mesh):
    n = mesh.shape["cp"]

    def local(x, seg, wq, wk, wv, wo):
        y, flag = _fused(x, seg, wq, wk, wv, wo)
        return lax.cond(flag[0, 0] > 0, lambda y: _general(x, seg, wq, wk, wv, wo, n), lambda y: y, y)

    rows = P(("dp", "cp"), None)
    return jax.shard_map(local, mesh=mesh, in_specs=(rows, P(("dp", "cp")), P(), P(), P(), P()), out_specs=rows, check_vma=False)
```

```python
import functools
import math

import jax
import jax.numpy as jnp
from jax import lax
from jax.experimental import pallas as pl
from jax.experimental.pallas import tpu as pltpu
from jax.sharding import PartitionSpec as P

DH = 128
NKV = 8
G = 4
PIECE = 128
CH = 4 * PIECE
R = G * PIECE
D = 4096
SCALE = math.log2(math.e) / math.sqrt(DH)
NEG = -1e30
MESH = pl.DeviceIdType.MESH
NWB = 5
N_SEND = (11, 15, 21, 17)
N_RECV = ((3, 4, 6, 3), (1, 2, 4, 3), (0, 0, 0, 2), (6, 8, 12, 10))


def _dot_t(a, b):
    return lax.dot_general(a, b, (((1,), (1,)), ((), ())), preferred_element_type=jnp.float32)


def _dot(a, b):
    return lax.dot_general(a, b, (((1,), (0,)), ((), ())), preferred_element_type=jnp.float32)


def _chunk_of(z, n):
    t = n - (z + 1)
    c_lo = jnp.where(n == 0, z, n - 1)
    c_far = jnp.where(t == 0, 4, jnp.where(t <= 4, t - 1, 5))
    c_near = jnp.where(t == 1, 5, 4)
    lo = t < 0
    c = jnp.where(lo, c_lo, jnp.where(z >= 2, c_far, c_near))
    return jnp.where(lo, 0, 1), c, (z >= 2) | (t <= 1)


def _mask(out_ref, me, own, low_query, seg_ref, dev, low_key, valid=True):
    def pick(low, both):
        return jnp.where(low, both[:1], both[1:])
    def piece(low, d):
        return jnp.where(low, d, 31 - d) * PIECE
    shape = (PIECE, PIECE)
    sq = jnp.transpose(jnp.broadcast_to(pick(low_query, own), shape))
    rows = lax.broadcasted_iota(jnp.int32, shape, 0) + piece(low_query, me)
    lanes = lax.broadcasted_iota(jnp.int32, shape, 1)
    for j in range(4):
        ok = (sq == pick(low_key, seg_ref[dev + j])) & (lanes + piece(low_key, dev + j) <= rows) & valid
        out_ref[:, j * PIECE:(j + 1) * PIECE] = jnp.where(ok, 0.0, NEG)


def _fused_kernel(x_ref, seg_ref, wk_ref, wv_ref, wq_ref, wo_ref, y_ref, flag_ref,
                  kv_ref, q_ref, w_ref, s_ref, bias_ref, m_ref, l_ref, acc_ref, yacc_ref, o_ref,
                  seg_all, seg_other, ssem, rsem, wsem, seg_lsem, seg_ssem, seg_rsem, seg_osem):
    me = lax.axis_index("cp")
    dp = lax.axis_index("dp")
    z = me // 4
    y = (me // 2) % 2
    c = me % 2
    yb = 1 - y
    to_y = 4 * z + 2 * yb + c
    to_c = 4 * z + 2 * y + (1 - c)

    def tile_copies(t):
        slot = lax.rem(t, NWB)
        buf, sem = w_ref.at[slot], wsem.at[slot]
        def kv_tile():
            return [pltpu.make_async_copy(w.at[:, pl.ds(pl.multiple_of(256 * t, 256), 256)], buf.at[:, pl.ds(256 * i, 256)], sem)
                    for i, w in enumerate((wk_ref, wv_ref))]
        def q_tile():
            return [pltpu.make_async_copy(wq_ref.at[:, pl.ds(pl.multiple_of(512 * (t - 4), 512), 512)], buf, sem)]
        def o_tile():
            return [pltpu.make_async_copy(wo_ref.at[pl.ds(pl.multiple_of(512 * (t - 12), 512), 512), pl.ds(512 * j, 512)],
                                          buf.at[pl.ds(512 * j, 512), :], sem) for j in range(8)]
        return kv_tile, q_tile, o_tile

    def start_tile(t):
        kv_tile, q_tile, o_tile = tile_copies(t)
        @pl.when(t < 4)
        def _():
            for cp in kv_tile():
                cp.start()
        @pl.when((t >= 4) & (t < 12))
        def _():
            for cp in q_tile():
                cp.start()
        @pl.when((t >= 12) & (t < 20))
        def _():
            for cp in o_tile():
                cp.start()

    def wait_tile(t):
        slot = lax.rem(t, NWB)
        pltpu.make_async_copy(wq_ref.at[:, pl.ds(0, 512)], w_ref.at[slot], wsem.at[slot]).wait()

    own_seg = pltpu.make_async_copy(seg_ref, seg_all.at[me], seg_lsem)
    own_seg.start()
    for t in range(NWB):
        start_tile(jnp.int32(t))

    barrier = pltpu.get_barrier_semaphore()
    for i in range(1, 16):
        pl.semaphore_signal(barrier, inc=1, device_id={"cp": lax.rem(me + i, 16)}, device_id_type=MESH)
    pl.semaphore_signal(barrier, inc=1, device_id={"dp": 1 - dp}, device_id_type=MESH)

    def enter(_):
        pl.semaphore_wait(barrier, 16)

    def share_seg(_):
        own_seg.wait()
        for i in range(1, 16):
            pltpu.make_async_remote_copy(src_ref=seg_all.at[me], dst_ref=seg_all.at[me], send_sem=seg_ssem, recv_sem=seg_rsem,
                                         device_id={"cp": lax.rem(me + i, 16)}, device_id_type=MESH).start()

    seg_swap = pltpu.make_async_remote_copy(src_ref=seg_all, dst_ref=seg_other, send_sem=seg_osem.at[0], recv_sem=seg_osem.at[1],
                                            device_id={"dp": 1 - dp}, device_id_type=MESH)

    def low(k, yy):
        return 4 * k + 2 * yy + c
    def own_high(yy):
        return 16 + 2 * yy + c
    def up_high(yy):
        return 20 + 2 * yy + c

    def send(h, stage, target, src, dst=None):
        dst = src if dst is None else dst
        pltpu.make_async_remote_copy(src_ref=kv_ref.at[h, src], dst_ref=kv_ref.at[h, dst], send_sem=ssem.at[h],
                                     recv_sem=rsem.at[h, stage], device_id={"cp": target}, device_id_type=MESH).start()

    def mate(h, *items):
        for i in items:
            send(h, 3, to_c, i)

    def t0(h):
        @pl.when(z == 0)
        def _():
            send(h, 0, me + 8, low(0, y))
            send(h, 0, me + 4, low(0, y))
            send(h, 0, to_y, low(0, y))
            send(h, 0, to_y, own_high(y))
            mate(h, low(0, y), own_high(y))
        for zz in (1, 2):
            @pl.when(z == zz)
            def _():
                send(h, 0, me + 4, low(zz, y))
                send(h, 0, to_y, low(zz, y))
                send(h, 0, to_y, own_high(y))
                send(h, 0, me - 4, own_high(y), up_high(y))
                mate(h, low(zz, y), own_high(y))
        @pl.when(z == 3)
        def _():
            send(h, 0, me - 4, low(3, y))
            send(h, 0, to_y, low(3, y))
            send(h, 0, to_y, own_high(y))
            send(h, 0, me - 4, own_high(y), up_high(y))
            mate(h, low(3, y), own_high(y))

    def arrive(h, stage):
        for zz in range(4):
            n = N_RECV[stage][zz]
            if n:
                @pl.when(z == zz)
                def _():
                    pltpu.make_async_copy(kv_ref.at[h, pl.ds(0, n)], kv_ref.at[h, pl.ds(0, n)], rsem.at[h, stage]).wait()

    def w1(h):
        arrive(h, 0)
        @pl.when(z == 0)
        def _():
            send(h, 1, to_y, up_high(y))
            mate(h, low(0, yb), own_high(yb), up_high(y))
        @pl.when(z == 1)
        def _():
            send(h, 1, me + 4, low(1, yb))
            send(h, 1, to_y, low(0, y))
            send(h, 1, to_y, up_high(y))
            mate(h, low(1, yb), own_high(yb), low(0, y), up_high(y))
        @pl.when(z == 2)
        def _():
            send(h, 1, me + 4, low(1, y))
            send(h, 1, me + 4, low(2, yb))
            send(h, 1, me + 4, low(0, y))
            send(h, 1, to_y, low(0, y))
            send(h, 1, to_y, up_high(y))
            mate(h, low(2, yb), low(1, y), low(0, y), up_high(y), own_high(yb), low(3, y))
        @pl.when(z == 3)
        def _():
            send(h, 1, me - 4, low(3, yb))
            mate(h, low(3, yb), own_high(yb), low(2, y))

    def w2(h):
        arrive(h, 1)
        @pl.when(z == 0)
        def _():
            mate(h, up_high(yb))
        @pl.when(z == 1)
        def _():
            mate(h, low(0, yb), up_high(yb))
        @pl.when(z == 2)
        def _():
            mate(h, low(1, yb), low(3, yb), low(0, yb), up_high(yb))
        @pl.when(z == 3)
        def _():
            send(h, 2, to_y, low(1, y))
            send(h, 2, to_y, low(0, y))
            mate(h, low(1, y), low(0, y), low(2, yb))

    def w3(h):
        arrive(h, 2)
        @pl.when(z == 3)
        def _():
            mate(h, low(0, yb), low(1, yb))

    def w4(h):
        arrive(h, 3)

    def kv_step(t):
        wait_tile(t)
        r = _dot(x_ref[...], w_ref[lax.rem(t, NWB)]).astype(jnp.bfloat16)
        for sel, slot in ((0, low(z, y)), (1, own_high(y))):
            for i in range(2):
                for j in range(2):
                    kv_ref[2 * t + i, slot, j] = r[sel * PIECE:(sel + 1) * PIECE, 256 * j + 128 * i:256 * j + 128 * (i + 1)]
        start_tile(t + NWB)

    def kv_body(t, _):
        kv_step(t)
        run(kv_plan, t)
        return 0

    def run(plan, i):
        for when, *what in plan:
            @pl.when(i == when)
            def _():
                for fn, head in what:
                    fn(head)

    kv_plan = (
        (0, (enter, 0), (t0, 0), (share_seg, 0)),
        (1, (t0, 1), (t0, 2)),
        (3, (w1, 0)),
    )
    lax.fori_loop(0, 4, kv_body, 0)

    def make_bias(_):
        pltpu.make_async_copy(seg_all.at[pl.ds(0, 15)], seg_all.at[pl.ds(0, 15)], seg_rsem).wait()
        seg_swap.start()
        own = seg_all[me]
        def body(n, _):
            sel, ck, valid = _chunk_of(z, n)
            low_key = ck < 4
            dev = jnp.where(low_key, 4 * ck, jnp.minimum(4 * (z + ck - 4), 12))
            _mask(bias_ref.at[n], me, own, sel == 0, seg_all, dev, low_key, valid)
            return 0
        lax.fori_loop(0, 3 * groups, body, 0)

    groups = jnp.where(z >= 2, 3, z + 1)

    def q_body(j, _):
        t = j + 4
        wait_tile(t)
        r = _dot(x_ref[...], w_ref[lax.rem(t, NWB)]).astype(jnp.bfloat16)
        for sel in range(2):
            for g in range(G):
                q_ref[j, sel, g * PIECE:(g + 1) * PIECE, :] = r[sel * PIECE:(sel + 1) * PIECE, g * DH:(g + 1) * DH]
        start_tile(t + NWB)
        run(q_plan, j)
        return 0

    q_plan = (
        (1, (w1, 1)),
        (2, (t0, 3)),
        (3, (w2, 0), (make_bias, 0)),
        (4, (w1, 2)),
        (7, (w2, 1), (w3, 0)),
    )
    lax.fori_loop(0, 8, q_body, 0)

    def score(h, n):
        sel, ck, _ = _chunk_of(z, n)
        k = kv_ref[h, pl.ds(4 * ck, 4), 0].reshape(CH, DH)
        s = _dot_t(q_ref[h, sel], k)
        s = (s.reshape(G, PIECE, CH) * SCALE + bias_ref[n][None]).reshape(R, CH)
        s_ref[n] = s
        s = [s[:, i * DH:(i + 1) * DH] for i in range(4)]
        m_ref[sel] = jnp.maximum(m_ref[sel], functools.reduce(jnp.maximum, s))

    def weigh(h, n):
        sel, ck, _ = _chunk_of(z, n)
        v = kv_ref[h, pl.ds(4 * ck, 4), 1].reshape(CH, DH)
        m = m_ref[sel]
        p = [jnp.exp2(s_ref[n, :, i * DH:(i + 1) * DH] - m) for i in range(4)]
        l_ref[sel] = l_ref[sel] + functools.reduce(jnp.add, p)
        pb = jnp.concatenate([a.astype(jnp.bfloat16) for a in p], axis=1)
        acc_ref[sel] = acc_ref[sel] + _dot(pb, v)

    def steps(fn, h, first, last):
        def group(i, _):
            for u in range(3):
                fn(h, 3 * i + u)
            return 0
        lax.fori_loop(first, last, group, 0)

    def project(t, last):
        slots = lax.rem(t, NWB), lax.rem(t + 1, NWB)
        for j in range(8):
            cols = slice(R * j, R * (j + 1))
            r = _dot(o_ref[0], w_ref[slots[0], cols, :]) + _dot(o_ref[1], w_ref[slots[1], cols, :])
            if last:
                y_ref[:, cols] = (yacc_ref[:, cols] + r).astype(jnp.bfloat16)
            else:
                yacc_ref[:, cols] = yacc_ref[:, cols] + r
        start_tile(t + NWB)
        start_tile(t + 1 + NWB)

    def attend(h, half, last=False):
        def ahead(n, fn):
            @pl.when(h + n < NKV)
            def _():
                fn(h + n)
        w4(h)
        m_ref[...] = jnp.full_like(m_ref, -jnp.inf)
        l_ref[...] = jnp.zeros_like(l_ref)
        acc_ref[...] = jnp.zeros_like(acc_ref)
        steps(score, h, 0, 1)
        if not last:
            ahead(4, t0)
        steps(score, h, 1, groups)
        if not last:
            ahead(3, w1)
        for sel in range(2):
            m_ref[sel] = jnp.broadcast_to(jnp.max(m_ref[sel], axis=1, keepdims=True), (R, DH))
        steps(weigh, h, 0, groups)
        if not last:
            ahead(1, w3)
            ahead(2, w2)
        t = h + 11
        if half:
            wait_tile(t)
            wait_tile(t + 1)
        for sel in range(2):
            a = (acc_ref[sel] / jnp.sum(l_ref[sel], axis=1, keepdims=True)).astype(jnp.bfloat16)
            for g in range(G):
                o_ref[half, sel * PIECE:(sel + 1) * PIECE, g * DH:(g + 1) * DH] = a[g * PIECE:(g + 1) * PIECE]
        if half:
            project(t, last)

    yacc_ref[...] = jnp.zeros_like(yacc_ref)

    def pair(i, _):
        attend(2 * i, 0)
        attend(2 * i + 1, 1)
        return 0
    lax.fori_loop(0, 3, pair, 0)
    attend(jnp.int32(6), 0)
    attend(jnp.int32(7), 1, last=True)

    seg_swap.wait()
    def reach(ref):
        def first(d):
            return jnp.broadcast_to(ref[d][1:2, 0:1], (1, PIECE))
        def last_(d):
            return jnp.broadcast_to(ref[d][1:2, PIECE - 1:PIECE], (1, PIECE))
        return (first(7) == last_(12)) | (first(3) == last_(8))
    flag_ref[...] = jnp.where(reach(seg_all) | reach(seg_other), 1, 0)

    pltpu.make_async_copy(seg_all.at[pl.ds(0, 15)], seg_all.at[pl.ds(0, 15)], seg_ssem).wait()
    def drain(h, _):
        for zz in range(4):
            @pl.when(z == zz)
            def _():
                ref = kv_ref.at[h, pl.ds(0, N_SEND[zz])]
                pltpu.make_async_copy(ref, ref, ssem.at[h]).wait()
        return 0
    lax.fori_loop(0, NKV, drain, 0)


def _fused(x, seg, wq, wk, wv, wo):
    vmem = pl.BlockSpec(memory_space=pltpu.VMEM)
    hbm = pl.BlockSpec(memory_space=pl.ANY)
    dma = pltpu.SemaphoreType.DMA
    return pl.pallas_call(
        _fused_kernel,
        out_shape=(jax.ShapeDtypeStruct((2 * PIECE, D), jnp.bfloat16), jax.ShapeDtypeStruct((1, PIECE), jnp.int32)),
        in_specs=[vmem, hbm, hbm, hbm, hbm, hbm],
        out_specs=(vmem, vmem),
        scratch_shapes=[
            pltpu.VMEM((NKV, 24, 2, PIECE, DH), jnp.bfloat16),
            pltpu.VMEM((NKV, 2, R, DH), jnp.bfloat16),
            pltpu.VMEM((NWB, D, 512), jnp.bfloat16),
            pltpu.VMEM((9, R, CH), jnp.float32),
            pltpu.VMEM((9, PIECE, CH), jnp.float32),
            pltpu.VMEM((2, R, DH), jnp.float32),
            pltpu.VMEM((2, R, DH), jnp.float32),
            pltpu.VMEM((2, R, DH), jnp.float32),
            pltpu.VMEM((2 * PIECE, D), jnp.float32),
            pltpu.VMEM((2, 2 * PIECE, R), jnp.bfloat16),
            pltpu.VMEM((16, 2, PIECE), jnp.int32),
            pltpu.VMEM((16, 2, PIECE), jnp.int32),
            dma((NKV,)),
            dma((NKV, 4)),
            dma((NWB,)),
            dma, dma, dma,
            dma((2,)),
        ],
        compiler_params=pltpu.CompilerParams(collective_id=0, has_side_effects=True, vmem_limit_bytes=67043328),
        cost_estimate=pl.CostEstimate(flops=30_000_000_000, bytes_accessed=90_000_000, transcendentals=0),
    )(x, seg.reshape(2, PIECE), wk, wv, wq, wo)


def _chunk_any(z, n):
    lo = n <= z
    t = n - (z + 1)
    c_lo = jnp.where(n == 0, z, n - 1)
    c_hi = jnp.where(t == 0, 4 + z, jnp.where(t <= 4, t - 1, z + t))
    return lo, jnp.where(lo, c_lo, c_hi)


def _any_kernel(q_ref, kv_ref, seg_ref, o_ref, bias_ref, m_ref, l_ref, acc_ref):
    me = lax.axis_index("cp")
    z = me // 4
    m_ref[...] = jnp.full_like(m_ref, -jnp.inf)
    l_ref[...] = jnp.zeros_like(l_ref)
    acc_ref[...] = jnp.zeros_like(acc_ref)
    own = seg_ref[me]

    def body(n, _):
        lo, ck = _chunk_any(z, n)
        sel = jnp.where(lo, 0, 1)
        hi = jnp.where(ck >= 4, 1, 0)
        dev0 = 4 * (ck - 4 * hi)
        _mask(bias_ref, me, own, lo, seg_ref, dev0, hi == 0)
        k = kv_ref[pl.ds(dev0, 4), hi, 0, 0].reshape(CH, DH)
        v = kv_ref[pl.ds(dev0, 4), hi, 0, 1].reshape(CH, DH)
        for g in range(G):
            i = sel * G + g
            s = _dot_t(q_ref[sel, 0, g], k) * SCALE + bias_ref[...]
            m_old = m_ref[i]
            m_new = jnp.maximum(m_old, jnp.max(s, axis=1, keepdims=True))
            p = jnp.exp2(s - m_new[:, :1])
            corr = jnp.exp2(m_old - m_new)
            l_ref[i] = l_ref[i] * corr + jnp.sum(p, axis=1, keepdims=True)
            acc_ref[i] = acc_ref[i] * corr + _dot(p.astype(jnp.bfloat16), v)
            m_ref[i] = m_new
        return 0
    lax.fori_loop(0, 9, body, 0)
    for sel in range(2):
        for g in range(G):
            o_ref[sel, 0, g] = (acc_ref[sel * G + g] / l_ref[sel * G + g]).astype(jnp.bfloat16)


def _general(x, seg, wq, wk, wv, wo, n):
    perm = [(j, (j + 1) % n) for j in range(n)]
    k = jnp.dot(x, wk, preferred_element_type=jnp.float32).astype(jnp.bfloat16)
    v = jnp.dot(x, wv, preferred_element_type=jnp.float32).astype(jnp.bfloat16)
    kv = jnp.stack([k.reshape(2, PIECE, NKV, DH), v.reshape(2, PIECE, NKV, DH)], axis=0)
    kv = jnp.transpose(kv, (1, 3, 0, 2, 4))
    seg = seg.reshape(2, PIECE)
    me = lax.axis_index("cp")

    def body(i, carry):
        kv, sg, kv_all, sg_all = carry
        src = (me - i) % n
        kv_all = lax.dynamic_update_index_in_dim(kv_all, kv, src, 0)
        sg_all = lax.dynamic_update_index_in_dim(sg_all, sg, src, 0)
        return lax.ppermute(kv, "cp", perm), lax.ppermute(sg, "cp", perm), kv_all, sg_all
    init = (kv, seg, jnp.zeros((n,) + kv.shape, kv.dtype), jnp.zeros((n,) + seg.shape, seg.dtype))
    _, _, kv_all, seg_all = lax.fori_loop(0, n, body, init)
    q = jnp.dot(x, wq, preferred_element_type=jnp.float32).astype(jnp.bfloat16)
    q = jnp.transpose(q.reshape(2, PIECE, NKV, G, DH), (0, 2, 3, 1, 4))
    o = pl.pallas_call(
        _any_kernel,
        out_shape=jax.ShapeDtypeStruct((2, NKV, G, PIECE, DH), jnp.bfloat16),
        grid=(NKV,),
        in_specs=[
            pl.BlockSpec((2, 1, G, PIECE, DH), lambda h: (0, h, 0, 0, 0)),
            pl.BlockSpec((n, 2, 1, 2, PIECE, DH), lambda h: (0, 0, h, 0, 0, 0)),
            pl.BlockSpec((n, 2, PIECE), lambda h: (0, 0, 0)),
        ],
        out_specs=pl.BlockSpec((2, 1, G, PIECE, DH), lambda h: (0, h, 0, 0, 0)),
        scratch_shapes=[pltpu.VMEM((PIECE, CH), jnp.float32)] + [pltpu.VMEM((2 * G, PIECE, DH), jnp.float32)] * 3,
    )(q, kv_all, seg_all)
    o = jnp.transpose(o, (0, 3, 1, 2, 4)).reshape(2 * PIECE, NKV * G * DH)
    return jnp.dot(o, wo, preferred_element_type=jnp.float32).astype(jnp.bfloat16)


def solution(mesh):
    n = mesh.shape["cp"]

    def local(x, seg, wq, wk, wv, wo):
        y, flag = _fused(x, seg, wq, wk, wv, wo)
        return lax.cond(flag[0, 0] > 0, lambda y: _general(x, seg, wq, wk, wv, wo, n), lambda y: y, y)

    rows = P(("dp", "cp"), None)
    return jax.shard_map(local, mesh=mesh, in_specs=(rows, P(("dp", "cp")), P(), P(), P(), P()), out_specs=rows, check_vma=False)
```

```python
import functools
import math

import jax
import jax.numpy as jnp
from jax import lax
from jax.experimental import pallas as pl
from jax.experimental.pallas import tpu as pltpu
from jax.sharding import PartitionSpec as P

DH = 128
NKV = 8
G = 4
PIECE = 128
CH = 4 * PIECE
R = G * PIECE
D = 4096
SCALE = math.log2(math.e) / math.sqrt(DH)
NEG = -1e30
MESH = pl.DeviceIdType.MESH
NWB = 5
N_SEND = (11, 15, 21, 17)
N_RECV = ((3, 4, 6, 3), (1, 2, 4, 3), (0, 0, 0, 2), (6, 8, 12, 10))


def _dot_t(a, b):
    return lax.dot_general(a, b, (((1,), (1,)), ((), ())), preferred_element_type=jnp.float32)


def _dot(a, b):
    return lax.dot_general(a, b, (((1,), (0,)), ((), ())), preferred_element_type=jnp.float32)


def _chunk_of(z, n):
    t = n - (z + 1)
    c_lo = jnp.where(n == 0, z, n - 1)
    c_far = jnp.where(t == 0, 4, jnp.where(t <= 4, t - 1, 5))
    c_near = jnp.where(t == 1, 5, 4)
    lo = t < 0
    c = jnp.where(lo, c_lo, jnp.where(z >= 2, c_far, c_near))
    return jnp.where(lo, 0, 1), c, (z >= 2) | (t <= 1)


def _mask(out_ref, me, own, low_query, seg_ref, dev, low_key, valid=True):
    def pick(low, both):
        return jnp.where(low, both[:1], both[1:])
    def piece(low, d):
        return jnp.where(low, d, 31 - d) * PIECE
    shape = (PIECE, PIECE)
    sq = jnp.transpose(jnp.broadcast_to(pick(low_query, own), shape))
    rows = lax.broadcasted_iota(jnp.int32, shape, 0) + piece(low_query, me)
    lanes = lax.broadcasted_iota(jnp.int32, shape, 1)
    for j in range(4):
        ok = (sq == pick(low_key, seg_ref[dev + j])) & (lanes + piece(low_key, dev + j) <= rows) & valid
        out_ref[:, j * PIECE:(j + 1) * PIECE] = jnp.where(ok, 0.0, NEG)


def _fused_kernel(x_ref, seg_ref, wk_ref, wv_ref, wq_ref, wo_ref, y_ref, flag_ref,
                  kv_ref, q_ref, w_ref, s_ref, bias_ref, m_ref, l_ref, acc_ref, yacc_ref, o_ref,
                  seg_all, seg_other, ssem, rsem, wsem, seg_lsem, seg_ssem, seg_rsem, seg_osem):
    me = lax.axis_index("cp")
    dp = lax.axis_index("dp")
    z = me // 4
    y = (me // 2) % 2
    c = me % 2
    yb = 1 - y
    to_y = 4 * z + 2 * yb + c
    to_c = 4 * z + 2 * y + (1 - c)

    def tile_copies(t):
        slot = lax.rem(t, NWB)
        buf, sem = w_ref.at[slot], wsem.at[slot]
        def kv_tile():
            return [pltpu.make_async_copy(w.at[:, pl.ds(pl.multiple_of(256 * t, 256), 256)], buf.at[:, pl.ds(256 * i, 256)], sem)
                    for i, w in enumerate((wk_ref, wv_ref))]
        def q_tile():
            return [pltpu.make_async_copy(wq_ref.at[:, pl.ds(pl.multiple_of(512 * (t - 4), 512), 512)], buf, sem)]
        def o_tile():
            return [pltpu.make_async_copy(wo_ref.at[pl.ds(pl.multiple_of(512 * (t - 12), 512), 512), pl.ds(512 * j, 512)],
                                          buf.at[pl.ds(512 * j, 512), :], sem) for j in range(8)]
        return kv_tile, q_tile, o_tile

    def start_tile(t):
        kv_tile, q_tile, o_tile = tile_copies(t)
        @pl.when(t < 4)
        def _():
            for cp in kv_tile():
                cp.start()
        @pl.when((t >= 4) & (t < 12))
        def _():
            for cp in q_tile():
                cp.start()
        @pl.when((t >= 12) & (t < 20))
        def _():
            for cp in o_tile():
                cp.start()

    def wait_tile(t):
        slot = lax.rem(t, NWB)
        pltpu.make_async_copy(wq_ref.at[:, pl.ds(0, 512)], w_ref.at[slot], wsem.at[slot]).wait()

    own_seg = pltpu.make_async_copy(seg_ref, seg_all.at[me], seg_lsem)
    own_seg.start()
    for t in range(NWB):
        start_tile(jnp.int32(t))

    barrier = pltpu.get_barrier_semaphore()
    for i in range(1, 16):
        pl.semaphore_signal(barrier, inc=1, device_id={"cp": lax.rem(me + i, 16)}, device_id_type=MESH)
    pl.semaphore_signal(barrier, inc=1, device_id={"dp": 1 - dp}, device_id_type=MESH)

    def enter(_):
        pl.semaphore_wait(barrier, 16)

    def share_seg(_):
        own_seg.wait()
        for i in range(1, 16):
            pltpu.make_async_remote_copy(src_ref=seg_all.at[me], dst_ref=seg_all.at[me], send_sem=seg_ssem, recv_sem=seg_rsem,
                                         device_id={"cp": lax.rem(me + i, 16)}, device_id_type=MESH).start()

    seg_swap = pltpu.make_async_remote_copy(src_ref=seg_all, dst_ref=seg_other, send_sem=seg_osem.at[0], recv_sem=seg_osem.at[1],
                                            device_id={"dp": 1 - dp}, device_id_type=MESH)

    def low(k, yy):
        return 4 * k + 2 * yy + c
    def own_high(yy):
        return 16 + 2 * yy + c
    def up_high(yy):
        return 20 + 2 * yy + c

    def send(h, stage, target, src, dst=None):
        dst = src if dst is None else dst
        pltpu.make_async_remote_copy(src_ref=kv_ref.at[h, src], dst_ref=kv_ref.at[h, dst], send_sem=ssem.at[h],
                                     recv_sem=rsem.at[h, stage], device_id={"cp": target}, device_id_type=MESH).start()

    def mate(h, *items):
        for i in items:
            send(h, 3, to_c, i)

    def t0(h):
        @pl.when(z == 0)
        def _():
            send(h, 0, me + 8, low(0, y))
            send(h, 0, me + 4, low(0, y))
            send(h, 0, to_y, low(0, y))
            send(h, 0, to_y, own_high(y))
            mate(h, low(0, y), own_high(y))
        for zz in (1, 2):
            @pl.when(z == zz)
            def _():
                send(h, 0, me + 4, low(zz, y))
                send(h, 0, to_y, low(zz, y))
                send(h, 0, to_y, own_high(y))
                send(h, 0, me - 4, own_high(y), up_high(y))
                mate(h, low(zz, y), own_high(y))
        @pl.when(z == 3)
        def _():
            send(h, 0, me - 4, low(3, y))
            send(h, 0, to_y, low(3, y))
            send(h, 0, to_y, own_high(y))
            send(h, 0, me - 4, own_high(y), up_high(y))
            mate(h, low(3, y), own_high(y))

    def arrive(h, stage):
        for zz in range(4):
            n = N_RECV[stage][zz]
            if n:
                @pl.when(z == zz)
                def _():
                    pltpu.make_async_copy(kv_ref.at[h, pl.ds(0, n)], kv_ref.at[h, pl.ds(0, n)], rsem.at[h, stage]).wait()

    def w1(h):
        arrive(h, 0)
        @pl.when(z == 0)
        def _():
            send(h, 1, to_y, up_high(y))
            mate(h, low(0, yb), own_high(yb), up_high(y))
        @pl.when(z == 1)
        def _():
            send(h, 1, me + 4, low(1, yb))
            send(h, 1, to_y, low(0, y))
            send(h, 1, to_y, up_high(y))
            mate(h, low(1, yb), own_high(yb), low(0, y), up_high(y))
        @pl.when(z == 2)
        def _():
            send(h, 1, me + 4, low(1, y))
            send(h, 1, me + 4, low(2, yb))
            send(h, 1, me + 4, low(0, y))
            send(h, 1, to_y, low(0, y))
            send(h, 1, to_y, up_high(y))
            mate(h, low(2, yb), low(1, y), low(0, y), up_high(y), own_high(yb), low(3, y))
        @pl.when(z == 3)
        def _():
            send(h, 1, me - 4, low(3, yb))
            mate(h, low(3, yb), own_high(yb), low(2, y))

    def w2(h):
        arrive(h, 1)
        @pl.when(z == 0)
        def _():
            mate(h, up_high(yb))
        @pl.when(z == 1)
        def _():
            mate(h, low(0, yb), up_high(yb))
        @pl.when(z == 2)
        def _():
            mate(h, low(1, yb), low(3, yb), low(0, yb), up_high(yb))
        @pl.when(z == 3)
        def _():
            send(h, 2, to_y, low(1, y))
            send(h, 2, to_y, low(0, y))
            mate(h, low(1, y), low(0, y), low(2, yb))

    def w3(h):
        arrive(h, 2)
        @pl.when(z == 3)
        def _():
            mate(h, low(0, yb), low(1, yb))

    def w4(h):
        arrive(h, 3)

    def kv_step(t):
        wait_tile(t)
        r = _dot(x_ref[...], w_ref[lax.rem(t, NWB)]).astype(jnp.bfloat16)
        for sel, slot in ((0, low(z, y)), (1, own_high(y))):
            for i in range(2):
                for j in range(2):
                    kv_ref[2 * t + i, slot, j] = r[sel * PIECE:(sel + 1) * PIECE, 256 * j + 128 * i:256 * j + 128 * (i + 1)]
        start_tile(t + NWB)

    def kv_body(t, _):
        kv_step(t)
        run(kv_plan, t)
        return 0

    def run(plan, i):
        for when, *what in plan:
            @pl.when(i == when)
            def _():
                for fn, head in what:
                    fn(head)

    kv_plan = (
        (0, (enter, 0), (t0, 0), (share_seg, 0)),
        (1, (t0, 1), (t0, 2)),
        (3, (w1, 0)),
    )
    yacc_ref[...] = jnp.zeros_like(yacc_ref)
    lax.fori_loop(0, 4, kv_body, 0)

    def make_bias(_):
        pltpu.make_async_copy(seg_all.at[pl.ds(0, 15)], seg_all.at[pl.ds(0, 15)], seg_rsem).wait()
        seg_swap.start()
        own = seg_all[me]
        def body(n, _):
            sel, ck, valid = _chunk_of(z, n)
            low_key = ck < 4
            dev = jnp.where(low_key, 4 * ck, jnp.minimum(4 * (z + ck - 4), 12))
            _mask(bias_ref.at[n], me, own, sel == 0, seg_all, dev, low_key, valid)
            return 0
        lax.fori_loop(0, 3 * groups, body, 0)

    groups = jnp.where(z >= 2, 3, z + 1)

    def q_body(j, _):
        t = j + 4
        wait_tile(t)
        r = _dot(x_ref[...], w_ref[lax.rem(t, NWB)]).astype(jnp.bfloat16)
        for sel in range(2):
            for g in range(G):
                q_ref[j, sel, g * PIECE:(g + 1) * PIECE, :] = r[sel * PIECE:(sel + 1) * PIECE, g * DH:(g + 1) * DH]
        start_tile(t + NWB)
        run(q_plan, j)
        return 0

    q_plan = (
        (1, (w1, 1)),
        (2, (t0, 3)),
        (3, (w2, 0), (make_bias, 0)),
        (4, (w1, 2)),
        (7, (w2, 1), (w3, 0)),
    )
    lax.fori_loop(0, 8, q_body, 0)

    def score(h, n):
        sel, ck, _ = _chunk_of(z, n)
        k = kv_ref[h, pl.ds(4 * ck, 4), 0].reshape(CH, DH)
        s = _dot_t(q_ref[h, sel], k)
        s = (s.reshape(G, PIECE, CH) * SCALE + bias_ref[n][None]).reshape(R, CH)
        s_ref[n] = s
        s = [s[:, i * DH:(i + 1) * DH] for i in range(4)]
        m_ref[sel] = jnp.maximum(m_ref[sel], functools.reduce(jnp.maximum, s))

    def weigh(h, n):
        sel, ck, _ = _chunk_of(z, n)
        v = kv_ref[h, pl.ds(4 * ck, 4), 1].reshape(CH, DH)
        m = m_ref[sel]
        p = [jnp.exp2(s_ref[n, :, i * DH:(i + 1) * DH] - m) for i in range(4)]
        l_ref[sel] = l_ref[sel] + functools.reduce(jnp.add, p)
        pb = jnp.concatenate([a.astype(jnp.bfloat16) for a in p], axis=1)
        acc_ref[sel] = acc_ref[sel] + _dot(pb, v)

    def steps(fn, h, first, last):
        def group(i, _):
            for u in range(3):
                fn(h, 3 * i + u)
            return 0
        lax.fori_loop(first, last, group, 0)

    def project(t, last):
        slots = lax.rem(t, NWB), lax.rem(t + 1, NWB)
        for j in range(8):
            cols = slice(R * j, R * (j + 1))
            r = _dot(o_ref[0], w_ref[slots[0], cols, :]) + _dot(o_ref[1], w_ref[slots[1], cols, :])
            if last:
                y_ref[:, cols] = (yacc_ref[:, cols] + r).astype(jnp.bfloat16)
            else:
                yacc_ref[:, cols] = yacc_ref[:, cols] + r
        start_tile(t + NWB)
        start_tile(t + 1 + NWB)

    def attend(h, half, last=False):
        def ahead(n, fn):
            @pl.when(h + n < NKV)
            def _():
                fn(h + n)
        w4(h)
        m_ref[...] = jnp.full_like(m_ref, -jnp.inf)
        l_ref[...] = jnp.zeros_like(l_ref)
        acc_ref[...] = jnp.zeros_like(acc_ref)
        steps(score, h, 0, 1)
        if not last:
            ahead(4, t0)
        steps(score, h, 1, groups)
        if not last:
            ahead(3, w1)
        for sel in range(2):
            m_ref[sel] = jnp.broadcast_to(jnp.max(m_ref[sel], axis=1, keepdims=True), (R, DH))
        steps(weigh, h, 0, groups)
        if not last:
            ahead(1, w3)
            ahead(2, w2)
        t = h + 11
        if half:
            wait_tile(t)
            wait_tile(t + 1)
        for sel in range(2):
            a = (acc_ref[sel] / jnp.sum(l_ref[sel], axis=1, keepdims=True)).astype(jnp.bfloat16)
            for g in range(G):
                o_ref[half, sel * PIECE:(sel + 1) * PIECE, g * DH:(g + 1) * DH] = a[g * PIECE:(g + 1) * PIECE]
        if half:
            project(t, last)


    def pair(i, _):
        attend(2 * i, 0)
        attend(2 * i + 1, 1)
        return 0
    lax.fori_loop(0, 3, pair, 0)
    attend(jnp.int32(6), 0)
    attend(jnp.int32(7), 1, last=True)

    seg_swap.wait()
    def reach(ref):
        def first(d):
            return jnp.broadcast_to(ref[d][1:2, 0:1], (1, PIECE))
        def last_(d):
            return jnp.broadcast_to(ref[d][1:2, PIECE - 1:PIECE], (1, PIECE))
        return (first(7) == last_(12)) | (first(3) == last_(8))
    flag_ref[...] = jnp.where(reach(seg_all) | reach(seg_other), 1, 0)

    pltpu.make_async_copy(seg_all.at[pl.ds(0, 15)], seg_all.at[pl.ds(0, 15)], seg_ssem).wait()
    def drain(h, _):
        for zz in range(4):
            @pl.when(z == zz)
            def _():
                ref = kv_ref.at[h, pl.ds(0, N_SEND[zz])]
                pltpu.make_async_copy(ref, ref, ssem.at[h]).wait()
        return 0
    lax.fori_loop(0, NKV, drain, 0)


def _fused(x, seg, wq, wk, wv, wo):
    vmem = pl.BlockSpec(memory_space=pltpu.VMEM)
    hbm = pl.BlockSpec(memory_space=pl.ANY)
    dma = pltpu.SemaphoreType.DMA
    return pl.pallas_call(
        _fused_kernel,
        out_shape=(jax.ShapeDtypeStruct((2 * PIECE, D), jnp.bfloat16), jax.ShapeDtypeStruct((1, PIECE), jnp.int32)),
        in_specs=[vmem, hbm, hbm, hbm, hbm, hbm],
        out_specs=(vmem, vmem),
        scratch_shapes=[
            pltpu.VMEM((NKV, 24, 2, PIECE, DH), jnp.bfloat16),
            pltpu.VMEM((NKV, 2, R, DH), jnp.bfloat16),
            pltpu.VMEM((NWB, D, 512), jnp.bfloat16),
            pltpu.VMEM((9, R, CH), jnp.float32),
            pltpu.VMEM((9, PIECE, CH), jnp.float32),
            pltpu.VMEM((2, R, DH), jnp.float32),
            pltpu.VMEM((2, R, DH), jnp.float32),
            pltpu.VMEM((2, R, DH), jnp.float32),
            pltpu.VMEM((2 * PIECE, D), jnp.float32),
            pltpu.VMEM((2, 2 * PIECE, R), jnp.bfloat16),
            pltpu.VMEM((16, 2, PIECE), jnp.int32),
            pltpu.VMEM((16, 2, PIECE), jnp.int32),
            dma((NKV,)),
            dma((NKV, 4)),
            dma((NWB,)),
            dma, dma, dma,
            dma((2,)),
        ],
        compiler_params=pltpu.CompilerParams(collective_id=0, has_side_effects=True, vmem_limit_bytes=67043328),
        cost_estimate=pl.CostEstimate(flops=30_000_000_000, bytes_accessed=90_000_000, transcendentals=0),
    )(x, seg.reshape(2, PIECE), wk, wv, wq, wo)


def _chunk_any(z, n):
    lo = n <= z
    t = n - (z + 1)
    c_lo = jnp.where(n == 0, z, n - 1)
    c_hi = jnp.where(t == 0, 4 + z, jnp.where(t <= 4, t - 1, z + t))
    return lo, jnp.where(lo, c_lo, c_hi)


def _any_kernel(q_ref, kv_ref, seg_ref, o_ref, bias_ref, m_ref, l_ref, acc_ref):
    me = lax.axis_index("cp")
    z = me // 4
    m_ref[...] = jnp.full_like(m_ref, -jnp.inf)
    l_ref[...] = jnp.zeros_like(l_ref)
    acc_ref[...] = jnp.zeros_like(acc_ref)
    own = seg_ref[me]

    def body(n, _):
        lo, ck = _chunk_any(z, n)
        sel = jnp.where(lo, 0, 1)
        hi = jnp.where(ck >= 4, 1, 0)
        dev0 = 4 * (ck - 4 * hi)
        _mask(bias_ref, me, own, lo, seg_ref, dev0, hi == 0)
        k = kv_ref[pl.ds(dev0, 4), hi, 0, 0].reshape(CH, DH)
        v = kv_ref[pl.ds(dev0, 4), hi, 0, 1].reshape(CH, DH)
        for g in range(G):
            i = sel * G + g
            s = _dot_t(q_ref[sel, 0, g], k) * SCALE + bias_ref[...]
            m_old = m_ref[i]
            m_new = jnp.maximum(m_old, jnp.max(s, axis=1, keepdims=True))
            p = jnp.exp2(s - m_new[:, :1])
            corr = jnp.exp2(m_old - m_new)
            l_ref[i] = l_ref[i] * corr + jnp.sum(p, axis=1, keepdims=True)
            acc_ref[i] = acc_ref[i] * corr + _dot(p.astype(jnp.bfloat16), v)
            m_ref[i] = m_new
        return 0
    lax.fori_loop(0, 9, body, 0)
    for sel in range(2):
        for g in range(G):
            o_ref[sel, 0, g] = (acc_ref[sel * G + g] / l_ref[sel * G + g]).astype(jnp.bfloat16)


def _general(x, seg, wq, wk, wv, wo, n):
    perm = [(j, (j + 1) % n) for j in range(n)]
    k = jnp.dot(x, wk, preferred_element_type=jnp.float32).astype(jnp.bfloat16)
    v = jnp.dot(x, wv, preferred_element_type=jnp.float32).astype(jnp.bfloat16)
    kv = jnp.stack([k.reshape(2, PIECE, NKV, DH), v.reshape(2, PIECE, NKV, DH)], axis=0)
    kv = jnp.transpose(kv, (1, 3, 0, 2, 4))
    seg = seg.reshape(2, PIECE)
    me = lax.axis_index("cp")

    def body(i, carry):
        kv, sg, kv_all, sg_all = carry
        src = (me - i) % n
        kv_all = lax.dynamic_update_index_in_dim(kv_all, kv, src, 0)
        sg_all = lax.dynamic_update_index_in_dim(sg_all, sg, src, 0)
        return lax.ppermute(kv, "cp", perm), lax.ppermute(sg, "cp", perm), kv_all, sg_all
    init = (kv, seg, jnp.zeros((n,) + kv.shape, kv.dtype), jnp.zeros((n,) + seg.shape, seg.dtype))
    _, _, kv_all, seg_all = lax.fori_loop(0, n, body, init)
    q = jnp.dot(x, wq, preferred_element_type=jnp.float32).astype(jnp.bfloat16)
    q = jnp.transpose(q.reshape(2, PIECE, NKV, G, DH), (0, 2, 3, 1, 4))
    o = pl.pallas_call(
        _any_kernel,
        out_shape=jax.ShapeDtypeStruct((2, NKV, G, PIECE, DH), jnp.bfloat16),
        grid=(NKV,),
        in_specs=[
            pl.BlockSpec((2, 1, G, PIECE, DH), lambda h: (0, h, 0, 0, 0)),
            pl.BlockSpec((n, 2, 1, 2, PIECE, DH), lambda h: (0, 0, h, 0, 0, 0)),
            pl.BlockSpec((n, 2, PIECE), lambda h: (0, 0, 0)),
        ],
        out_specs=pl.BlockSpec((2, 1, G, PIECE, DH), lambda h: (0, h, 0, 0, 0)),
        scratch_shapes=[pltpu.VMEM((PIECE, CH), jnp.float32)] + [pltpu.VMEM((2 * G, PIECE, DH), jnp.float32)] * 3,
    )(q, kv_all, seg_all)
    o = jnp.transpose(o, (0, 3, 1, 2, 4)).reshape(2 * PIECE, NKV * G * DH)
    return jnp.dot(o, wo, preferred_element_type=jnp.float32).astype(jnp.bfloat16)


def solution(mesh):
    n = mesh.shape["cp"]

    def local(x, seg, wq, wk, wv, wo):
        y, flag = _fused(x, seg, wq, wk, wv, wo)
        return lax.cond(flag[0, 0] > 0, lambda y: _general(x, seg, wq, wk, wv, wo, n), lambda y: y, y)

    rows = P(("dp", "cp"), None)
    return jax.shard_map(local, mesh=mesh, in_specs=(rows, P(("dp", "cp")), P(), P(), P(), P()), out_specs=rows, check_vma=False)
```
